32 devices in a mesh: gz: 32 (over z, y, x, core).
Axes of the slice: x: 2, y: 2, z: 4, core: 2. Of those that a mesh axis runs over, the one named last changes fastest.
Arguments:
- u_face: float32 [64, 1024, 512], P('gz')
- v_face: float32 [64, 1024, 512], P('gz')
- w_face: float32 [64, 1024, 512], P('gz')
- smoke: float32 [64, 1024, 512], P('gz'), may hold values from 0 to 2
- obstacles: int32 [64, 32, 512], P('gz'), may hold values from -2147483648 to 2147483647, as said below
Outputs:
- impulse: float32 [64, 1024, 512], P('gz')
- relative_residual: float32 [64, 1024, 512], P('gz')
The draws below stay inside these ranges and needn't reach their ends.
Inputs may be any that keep to these rules, and one draw needn't show every extreme that they name: Bit k of obstacles[z, b, x] is 1 where cell (z, 32 b + k, x) is solid and 0 where it holds fluid; every bit of a word is used.
All inputs are finite; a program needn't handle non-finite values. Where the reference program divides by a largest or mean magnitude, that divisor is 1e-20 or more.
Results may differ from the reference program's by a relative error of at most 0.00011.
Values sent between devices are 32-bit elements; how exact they have to be, the bound alone decides.
A program may use at most 192 MiB of HBM per device.

```python
import jax
import jax.numpy as jnp
from jax import lax

NX = 512
NY = 1024
ITERS = 2
NZ = 64


def velocity_field(key):
    first = jax.random.fold_in(key, 0)
    depth = jnp.arange(NZ, dtype=jnp.float32) / max(NZ - 1, 1)
    ramp = 1.0 + 2.0 * depth[:, None, None]
    base = jax.random.normal(first, (NZ, NY, NX), jnp.float32)
    return jnp.clip(base, -6.0, 6.0) * ramp


def draw_u_face(key, part):
    return velocity_field(jax.random.fold_in(key, 11))


def draw_v_face(key, part):
    return velocity_field(jax.random.fold_in(key, 23))


def draw_w_face(key, part):
    return velocity_field(jax.random.fold_in(key, 37))


def draw_obstacles(key, part):
    first, second = jax.random.split(jax.random.fold_in(key, 53))
    shape = (NZ, NY // 32, NX)
    left = jax.random.randint(first, shape, -2147483648, 2147483647, dtype=jnp.int32)
    right = jax.random.randint(second, shape, -2147483648, 2147483647, dtype=jnp.int32)
    return left & right


def levels(stream_key, shape, cuts, smallest, largest):
    gain, own = 1.0, jax.random.fold_in(stream_key, 6)
    for position, blocks in cuts:
        steps = jnp.exp(jax.random.uniform(jax.random.fold_in(own, position), (blocks,), jnp.float32, smallest / len(cuts), largest / len(cuts)))
        gain = gain * jnp.repeat(steps, shape[position] // blocks).reshape([-1 if axis == position else 1 for axis in range(len(shape))])
    return gain


def setup_inputs(seed: int = 0) -> dict:
    splits = jax.random.split(jax.random.key(seed), 6)
    return {
        "u_face": draw_u_face(jax.random.fold_in(splits[5], 71), 0),
        "v_face": draw_v_face(jax.random.fold_in(splits[5], 71), 0),
        "w_face": draw_w_face(jax.random.fold_in(splits[5], 71), 0),
        "smoke": jnp.clip(2.0 * jax.random.uniform(splits[3], (NZ, NY, NX), jnp.float32) ** levels(splits[3], (NZ, NY, NX), ((0, 32),), -0.2, 0.2), 0.0, 2.0),
        "obstacles": draw_obstacles(jax.random.fold_in(splits[5], 71), 0),
    }


EPS = 1e-06
CFL = 0.5
BUOYANCY = 100.0

def unpack_flags(packed):
    places = jnp.arange(32, dtype=jnp.int32)
    flags = jnp.right_shift(packed[:, :, None, :], places[None, None, :, None]) & 1
    return flags.reshape(packed.shape[0], packed.shape[1] * 32, packed.shape[2])

def next_along(field, axis):
    widths = [(0, 0), (0, 0), (0, 0)]
    widths[axis] = (0, 1)
    padded = jnp.pad(field, widths)
    return lax.slice_in_dim(padded, 1, field.shape[axis] + 1, axis=axis)

def neighbour_sum(field):
    padded = jnp.pad(field, 1)
    total = padded[2:, 1:-1, 1:-1] + padded[:-2, 1:-1, 1:-1]
    total = total + padded[1:-1, 2:, 1:-1] + padded[1:-1, :-2, 1:-1]
    return total + padded[1:-1, 1:-1, 2:] + padded[1:-1, 1:-1, :-2]

def reference(u_face, v_face, w_face, smoke, obstacles):
    solid_cells = unpack_flags(obstacles).astype(jnp.float32)
    fluid_cells = 1.0 - solid_cells
    fastest = jnp.maximum(jnp.maximum(jnp.max(jnp.abs(u_face)), jnp.max(jnp.abs(v_face))), jnp.max(jnp.abs(w_face)))
    time_step = CFL / (fastest + EPS)
    lift = time_step * BUOYANCY
    lifted_w = w_face + lift * smoke
    divergence = fluid_cells * (next_along(u_face, 2) - u_face + (next_along(v_face, 1) - v_face) + (next_along(lifted_w, 0) - lifted_w))
    div_squares = jnp.sum(divergence * divergence)
    fluid_total = jnp.maximum(jnp.sum(fluid_cells), 1.0)
    open_count = 6.0 - neighbour_sum(solid_cells)
    scaling = fluid_cells * jnp.maximum(open_count, 1.0) + solid_cells

    def apply_operator(search):
        return fluid_cells * (open_count * search - neighbour_sum(fluid_cells * search)) + solid_cells * search
    residual = divergence / time_step
    solution = jnp.zeros_like(residual)
    search = residual / scaling
    rz_now = jnp.sum(residual * residual / scaling)
    for step in range(ITERS):
        image = apply_operator(search)
        alpha = rz_now / jnp.sum(search * image)
        solution = solution + alpha * search
        residual = residual - alpha * image
        if step + 1 < ITERS:
            precond = residual / scaling
            rz_next = jnp.sum(residual * precond)
            search = precond + rz_next / rz_now * search
            rz_now = rz_next
    impulse = time_step * solution
    relative_residual = residual * time_step / jnp.sqrt(div_squares / fluid_total + EPS)
    return (impulse, relative_residual)
```

```python
import functools

import jax
import jax.numpy as jnp
from jax import lax
from jax.experimental import pallas as pl
from jax.experimental.pallas import tpu as pltpu
from jax.sharding import PartitionSpec as P

EPS = 1e-06
CFL = 0.5
BUOYANCY = 100.0

ROWS = 32
PAD = 8


def kernel(n, chunks, u_hbm, v_hbm, w_hbm, s_hbm, ob_hbm, imp_hbm, res_hbm,
           u, v, w, s, z, y, code, ay, lw, lw_next, ob, cw, acc, cf, mx, mx_all, st, st_all,
           in_sem, ob_send, ob_recv, lw_send, lw_recv, dn_send, dn_recv, up_send, up_recv,
           mx_send, mx_recv, st_send, st_recv, out_sem):
    depth, ny, nx = w.shape
    nb = ny // ROWS
    crow = ny // chunks
    me = lax.axis_index("gz")
    has_low, has_high = me > 0, me < n - 1
    low, high = jnp.maximum(me - 1, 0), jnp.minimum(me + 1, n - 1)

    def at(device):
        return dict(device_id=(device,), device_id_type=pl.DeviceIdType.MESH)

    ins = [(u_hbm, u), (v_hbm, v), (w_hbm, w), (s_hbm, s)]

    def load(k, p):
        src, dst = ins[k]
        return pltpu.make_async_copy(src.at[p], dst.at[p, pl.ds(0, ny)], in_sem.at[k * depth + p])

    ob_in = pltpu.make_async_copy(ob_hbm, ob.at[pl.ds(2, depth)], in_sem.at[4 * depth])
    ob_in.start()
    for k in range(4):
        for p in range(depth):
            load(k, p).start()

    barrier = pltpu.get_barrier_semaphore()

    def greet(i, carry):
        pl.semaphore_signal(barrier, inc=1, **at(lax.rem(me + i, n)))
        return carry

    lax.fori_loop(1, n, greet, 0)

    zrow = jnp.zeros((PAD, nx), jnp.float32)
    for p in range(depth + 4):
        z[p, 0:PAD, :] = zrow
        z[p, ny + PAD : ny + 2 * PAD, :] = zrow
    for p in range(depth + 2):
        y[p, 0:PAD, :] = zrow
        y[p, ny + PAD : ny + 2 * PAD, :] = zrow
    for p in range(depth):
        v[p, ny : ny + PAD, :] = zrow
    acc[...] = jnp.zeros_like(acc)

    def zero_planes(ref, planes, offset):
        def body(i, carry):
            for p in planes:
                ref[p, pl.ds(pl.multiple_of(i * ROWS + offset, 8), ROWS), :] = jnp.zeros((ROWS, nx), jnp.float32)
            return carry
        lax.fori_loop(0, nb, body, 0)

    ob_in.wait()
    pl.semaphore_wait(barrier, n - 1)

    ob_down = pltpu.make_async_remote_copy(
        ob.at[pl.ds(2, 2)], ob.at[pl.ds(depth + 2, 2)], ob_send.at[0], ob_recv.at[0], **at(low))
    ob_up = pltpu.make_async_remote_copy(
        ob.at[pl.ds(depth, 2)], ob.at[pl.ds(0, 2)], ob_send.at[1], ob_recv.at[1], **at(high))

    @pl.when(has_low)
    def _():
        ob_down.start()

    @pl.when(has_high)
    def _():
        ob_up.start()

    @pl.when(jnp.logical_not(has_low))
    def _():
        ob[0:2] = jnp.zeros((2,) + ob.shape[1:], jnp.int32)
        zero_planes(z, (0, 1), PAD)

    @pl.when(jnp.logical_not(has_high))
    def _():
        ob[depth + 2 : depth + 4] = jnp.zeros((2,) + ob.shape[1:], jnp.int32)
        zero_planes(z, (depth + 2, depth + 3), PAD)
        zero_planes(lw_next, (0,), 0)

    mx[...] = jnp.zeros_like(mx)
    for k in range(3):
        ref = ins[k][1]
        for p in range(depth):
            load(k, p).wait()

            def body(i, m, ref=ref, p=p):
                a = jnp.abs(ref[p, pl.ds(pl.multiple_of(i * ROWS, 8), ROWS), :])
                return jnp.maximum(m, jnp.max(a.reshape(ROWS // 8, 8, nx), axis=0))

            m = lax.fori_loop(0, nb, body, jnp.zeros((8, nx), jnp.float32))
            m = jnp.max(m, axis=0, keepdims=True)
            for c in range(0, nx, 128):
                mx[...] = jnp.maximum(mx[...], jnp.broadcast_to(m[:, c : c + 128], mx.shape))

    def spread(src, dst, send, recv):
        def copy(i):
            return pltpu.make_async_remote_copy(
                src, dst.at[i], send.at[i], recv.at[i], **at(lax.rem(me + i, n)))

        def start(i, carry):
            copy(i).start()
            return carry

        def wait(i, carry):
            copy(i).wait_recv()
            copy(i).wait_send()
            return carry

        return (lambda: lax.fori_loop(1, n, start, 0)), (lambda: lax.fori_loop(1, n, wait, 0))

    mx_start, mx_wait = spread(mx, mx_all, mx_send, mx_recv)
    mx_start()

    @pl.when(has_low)
    def _():
        ob_down.wait_send()
        ob_up.wait_recv()

    @pl.when(has_high)
    def _():
        ob_up.wait_send()
        ob_down.wait_recv()

    row_id = lax.broadcasted_iota(jnp.int32, (nb, nx), 0)
    col_id = lax.broadcasted_iota(jnp.int32, (nb, nx), 1)
    srl = lax.shift_right_logical
    c1, c31 = jnp.int32(1), jnp.int32(31)
    full1, full31 = jnp.full((nb, nx), c1), jnp.full((nb, nx), c31)
    for p in range(depth + 2):
        mid = ob[p + 1]
        after = jnp.where(row_id == nb - 1, 0, pltpu.roll(mid, nb - 1, 0))
        before = jnp.where(row_id == 0, 0, pltpu.roll(mid, 1, 0))
        a = srl(mid, full1) | (after << full31)
        b = (mid << full1) | srl(before, full31)
        c = jnp.where(col_id == nx - 1, 0, pltpu.roll(mid, nx - 1, 1))
        d = jnp.where(col_id == 0, 0, pltpu.roll(mid, 1, 1))
        e, f = ob[p], ob[p + 2]
        s1, k1 = a ^ b ^ c, (a & b) | (c & (a | b))
        s2, k2 = d ^ e ^ f, (d & e) | (f & (d | e))
        k3 = s1 & s2
        cw[p, 0] = s1 ^ s2
        cw[p, 1] = k1 ^ k2 ^ k3
        cw[p, 2] = (k1 & k2) | (k3 & (k1 | k2))
        outside = None
        if p == 0:
            outside = jnp.logical_not(has_low)
        if p == depth + 1:
            outside = jnp.logical_not(has_high)
        cw[p, 3] = mid
        if outside is not None:
            @pl.when(outside)
            def _(p=p):
                cw[p, 3] = jnp.full((nb, nx), -1, jnp.int32)

    half = 16
    places = lax.broadcasted_iota(jnp.int32, (half, nx), 0)

    def code_rows(b, carry):
        for p in range(depth + 2):
            for k0 in range(0, ROWS, half):
                bits = [
                    srl(jnp.broadcast_to(cw[p, j, pl.ds(b, 1), :], (half, nx)), places + k0) & 1
                    for j in range(4)
                ]
                count = bits[0] + (bits[1] << 1) + (bits[2] << 2)
                code[p, pl.ds(pl.multiple_of(b * ROWS + k0, 8), half), :] = jnp.where(
                    bits[3] == 1, -1, 6 - count).astype(jnp.float32)
        return carry

    lax.fori_loop(0, nb, code_rows, 0)

    for p in range(depth):
        load(3, p).wait()
    mx_wait()
    mx_all[0] = mx[...]
    top = jnp.max(jnp.max(mx_all[...], axis=0), axis=1, keepdims=True)[0:1]
    top = jnp.broadcast_to(top, (1, nx))
    cf[0:1, :] = (CFL / (top + EPS)) * BUOYANCY

    lane = lax.broadcasted_iota(jnp.int32, (ROWS, nx), 1)

    def lifted(p, r):
        rows = pl.ds(r, ROWS)
        return w[p, rows, :] + cf[0:1, :] * s[p, rows, :]

    def chunked(prepare, compute, sends):
        def body(c, carry):
            @pl.when(c < chunks)
            def _():
                prepare(c)

                def inner(i, k):
                    compute(pl.multiple_of(c * crow + i * ROWS, 8))
                    return k
                lax.fori_loop(0, crow // ROWS, inner, 0)

            @pl.when(c > 0)
            def _():
                for cond, copy in sends:
                    @pl.when(cond)
                    def _(copy=copy):
                        copy(c - 1).start()
            return carry
        lax.fori_loop(0, chunks + 1, body, 0)

    def lw_copy(c):
        rows = pl.ds(pl.multiple_of(c * crow, 8), crow)
        return pltpu.make_async_remote_copy(
            lw.at[0, rows], lw_next.at[0, rows], lw_send.at[c], lw_recv.at[c], **at(low))

    def lw_rows(r):
        lw[0, pl.ds(r, ROWS), :] = lifted(0, r)

    chunked(lambda c: None, lw_rows, [(has_low, lw_copy)])

    def z_copy(src, dst, send, recv, base, device):
        def copy(c):
            rows = pl.ds(pl.multiple_of(c * crow + PAD, 8), crow)
            return pltpu.make_async_remote_copy(
                z.at[src, rows], z.at[dst, rows], send.at[base + c], recv.at[base + c], **at(device))
        return copy

    down = [z_copy(2 + j, depth + 2 + j, dn_send, dn_recv, j * chunks, low) for j in range(2)]
    up = [z_copy(depth + j, j, up_send, up_recv, j * chunks, high) for j in range(2)]

    def z_rows(p, r):
        rows = pl.ds(r, ROWS)
        a = u[p, rows, :]
        flat = jnp.where(lane == nx - 1, 0.0, pltpu.roll(a, nx - 1, 1)) - a
        b = v[p, pl.ds(r, ROWS + PAD), :]
        flat = flat + (b[1 : ROWS + 1] - b[:ROWS])
        above = lifted(p + 1, r) if p + 1 < depth else lw_next[0, rows, :]
        own = lw[0, rows, :] if p == 0 else lifted(p, r)
        div = flat + (above - own)
        k = code[p + 1, rows, :]
        z[p + 2, pl.ds(pl.multiple_of(r + PAD, 8), ROWS), :] = (
            jnp.where(k >= 0.0, div, 0.0) / jnp.maximum(k, 1.0))

    for p in range(depth):
        def prepare(c, p=p):
            if p == depth - 1:
                @pl.when(has_high)
                def _():
                    lw_copy(c).wait_recv()
        sends = []
        if p < 2:
            sends.append((has_low, down[p]))
        if p >= depth - 2:
            sends.append((has_high, up[p - (depth - 2)]))
        chunked(prepare, functools.partial(z_rows, p), sends)

    def wait_all(cond, copy):
        def body(c, carry):
            @pl.when(cond)
            def _():
                copy(c).wait_recv()
            return carry
        lax.fori_loop(0, chunks, body, 0)

    def image(ref, slot, zm, zp, r, k):
        x = ref[slot, pl.ds(r, ROWS + 2 * PAD), :]
        mid = x[PAD : PAD + ROWS]
        beside = x[PAD + 1 : PAD + 1 + ROWS] + x[PAD - 1 : PAD - 1 + ROWS]
        beside = beside + jnp.where(lane == nx - 1, 0.0, pltpu.roll(mid, nx - 1, 1))
        beside = beside + jnp.where(lane == 0, 0.0, pltpu.roll(mid, 1, 1))
        beside = beside + zm + zp
        return mid, jnp.where(k >= 0.0, k * mid - beside, mid)

    def add(j, x):
        acc[j] += jnp.sum(x.reshape(ROWS // 8, 8, nx), axis=0)

    def y_rows(p, r):
        inner = pl.ds(pl.multiple_of(r + PAD, 8), ROWS)
        k = code[p + 1, pl.ds(r, ROWS), :]
        mid, q = image(z, p + 2, z[p + 1, inner, :], z[p + 3, inner, :], r, k)
        scaling = jnp.maximum(k, 1.0)
        out = q / scaling
        y[p + 1, inner, :] = out
        if 0 <= p < depth:
            d = scaling * mid
            add(0, d * mid)
            add(1, d * d)
            add(2, jnp.where(k >= 0.0, 1.0, 0.0))
            add(3, mid * q)
            add(4, q * out)

    def a_rows(p, r):
        inner = pl.ds(pl.multiple_of(r + PAD, 8), ROWS)
        k = code[p + 1, pl.ds(r, ROWS), :]
        mid, q = image(y, p + 1, y[p, inner, :], y[p + 2, inner, :], r, k)
        ay[p, pl.ds(r, ROWS), :] = q
        add(5, mid * q)

    def sweep(fn):
        def body(i, carry):
            fn(pl.multiple_of(i * ROWS, 8))
            return carry
        lax.fori_loop(0, nb, body, 0)

    wait_all(has_low, up[0])
    for p in range(depth - 1):
        if p == 0:
            wait_all(has_low, up[1])
            sweep(functools.partial(y_rows, -1))
        sweep(functools.partial(y_rows, p))
    wait_all(has_high, down[0])
    sweep(functools.partial(y_rows, depth - 1))
    for p in range(depth - 1):
        sweep(functools.partial(a_rows, p))

    def last_wait(c):
        @pl.when(has_high)
        def _():
            down[1](c).wait_recv()

    def last_rows(r):
        y_rows(depth, r)
        a_rows(depth - 1, r)

    chunked(last_wait, last_rows, [])

    for j in range(6):
        t = jnp.sum(acc[j], axis=0, keepdims=True)
        part = t[:, 0:128]
        for c in range(128, nx, 128):
            part = part + t[:, c : c + 128]
        st[j : j + 1, :] = part
    st[6:8, :] = jnp.zeros((2, 128), jnp.float32)
    st_start, st_wait = spread(st, st_all, st_send, st_recv)
    st_start()

    def drain(c, carry):
        @pl.when(has_low)
        def _():
            lw_copy(c).wait_send()
            down[0](c).wait_send()
            down[1](c).wait_send()

        @pl.when(has_high)
        def _():
            up[0](c).wait_send()
            up[1](c).wait_send()
        return carry

    lax.fori_loop(0, chunks, drain, 0)
    st_wait()
    st_all[0] = st[...]
    total = jnp.sum(jnp.sum(st_all[...], axis=0), axis=1, keepdims=True)
    total = jnp.broadcast_to(total, (8, nx))
    gamma, squares, fluid = total[0:1], total[1:2], total[2:3]
    delta, eta, theta = total[3:4], total[4:5], total[5:6]
    alpha = gamma / delta
    gamma_next = gamma - 2.0 * alpha * delta + alpha * alpha * eta
    beta = gamma_next / gamma
    mixed = delta - alpha * eta
    curve = (delta - 2.0 * alpha * eta + alpha * alpha * theta) + 2.0 * beta * mixed + beta * beta * delta
    alpha_next = gamma_next / curve
    cf[1:2, :] = alpha + alpha_next * (1.0 + beta)
    cf[2:3, :] = alpha * alpha_next
    cf[3:4, :] = 1.0 / jnp.sqrt(squares / jnp.maximum(fluid, 1.0) + EPS)

    def out_copy(p, c, j):
        rows = pl.ds(pl.multiple_of(c * crow, 8), crow)
        src, dst = ((w, imp_hbm), (s, res_hbm))[j]
        return pltpu.make_async_copy(src.at[p, rows], dst.at[p, rows], out_sem.at[j * depth + p, c])

    for p in range(depth):
        def out_rows(r, p=p):
            inner = pl.ds(pl.multiple_of(r + PAD, 8), ROWS)
            rows = pl.ds(r, ROWS)
            zz, yy = z[p + 2, inner, :], y[p + 1, inner, :]
            scaling = jnp.maximum(code[p + 1, rows, :], 1.0)
            a, b = cf[1:2, :], cf[2:3, :]
            w[p, rows, :] = a * zz - b * yy
            s[p, rows, :] = (scaling * (zz - a * yy) + b * ay[p, rows, :]) * cf[3:4, :]

        chunked(lambda c: None, out_rows,
                [(True, lambda c, p=p: out_copy(p, c, 0)), (True, lambda c, p=p: out_copy(p, c, 1))])

    def finish(c, carry):
        for p in range(depth):
            for j in range(2):
                out_copy(p, c, j).wait()
        return carry

    lax.fori_loop(0, chunks, finish, 0)


def solution(mesh):
    n = mesh.shape["gz"]

    def local(u_face, v_face, w_face, smoke, obstacles):
        depth, ny, nx = u_face.shape
        nw = obstacles.shape[1]
        chunks = 8
        f32, i32 = jnp.float32, jnp.int32
        dma = pltpu.SemaphoreType.DMA
        any_spec = pl.BlockSpec(memory_space=pl.ANY)
        shape = jax.ShapeDtypeStruct((depth, ny, nx), f32)
        return pl.pallas_call(
            functools.partial(kernel, n, chunks),
            out_shape=(shape, shape),
            in_specs=[any_spec] * 5,
            out_specs=(any_spec, any_spec),
            scratch_shapes=[
                pltpu.VMEM((depth, ny, nx), f32),
                pltpu.VMEM((depth, ny + PAD, nx), f32),
                pltpu.VMEM((depth, ny, nx), f32),
                pltpu.VMEM((depth, ny, nx), f32),
                pltpu.VMEM((depth + 4, ny + 2 * PAD, nx), f32),
                pltpu.VMEM((depth + 2, ny + 2 * PAD, nx), f32),
                pltpu.VMEM((depth + 2, ny, nx), f32),
                pltpu.VMEM((depth, ny, nx), f32),
                pltpu.VMEM((1, ny, nx), f32),
                pltpu.VMEM((1, ny, nx), f32),
                pltpu.VMEM((depth + 4, nw, nx), i32),
                pltpu.VMEM((depth + 2, 4, nw, nx), i32),
                pltpu.VMEM((6, 8, nx), f32),
                pltpu.VMEM((8, nx), f32),
                pltpu.VMEM((8, 128), f32),
                pltpu.VMEM((n, 8, 128), f32),
                pltpu.VMEM((8, 128), f32),
                pltpu.VMEM((n, 8, 128), f32),
                dma((4 * depth + 1,)),
                dma((2,)), dma((2,)),
                dma((chunks,)), dma((chunks,)),
                dma((2 * chunks,)), dma((2 * chunks,)),
                dma((2 * chunks,)), dma((2 * chunks,)),
                dma((n,)), dma((n,)),
                dma((n,)), dma((n,)),
                dma((2 * depth, chunks)),
            ],
            compiler_params=pltpu.CompilerParams(
                collective_id=0, has_side_effects=True, vmem_limit_bytes=66_000_000),
            name="smoke_step",
        )(u_face, v_face, w_face, smoke, obstacles)

    placed = P("gz", None, None)
    return jax.shard_map(local, mesh=mesh, in_specs=(placed,) * 5, out_specs=(placed, placed), check_vma=False)
```

```python
import functools

import jax
import jax.numpy as jnp
from jax import lax
from jax.experimental import pallas as pl
from jax.experimental.pallas import tpu as pltpu
from jax.sharding import PartitionSpec as P

EPS = 1e-06
CFL = 0.5
BUOYANCY = 100.0

ROWS = 32
PAD = 8


def kernel(n, chunks, u_hbm, v_hbm, w_hbm, s_hbm, ob_hbm, imp_hbm, res_hbm,
           u, v, w, s, z, y, code, ay, lw, lw_next, ob, cw, acc, cf, mx, mx_all, st, st_all,
           in_sem, ob_send, ob_recv, lw_send, lw_recv, dn_send, dn_recv, up_send, up_recv,
           mx_send, mx_recv, st_send, st_recv, out_sem):
    depth, ny, nx = w.shape
    nb = ny // ROWS
    crow = ny // chunks
    me = lax.axis_index("gz")
    has_low, has_high = me > 0, me < n - 1
    low, high = jnp.maximum(me - 1, 0), jnp.minimum(me + 1, n - 1)

    def at(device):
        return dict(device_id=(device,), device_id_type=pl.DeviceIdType.MESH)

    ins = [(u_hbm, u), (v_hbm, v), (w_hbm, w), (s_hbm, s)]

    def load(k, p):
        src, dst = ins[k]
        return pltpu.make_async_copy(src.at[p], dst.at[p, pl.ds(0, ny)], in_sem.at[k * depth + p])

    ob_in = pltpu.make_async_copy(ob_hbm, ob.at[pl.ds(2, depth)], in_sem.at[4 * depth])
    ob_in.start()
    for k in range(4):
        for p in range(depth):
            load(k, p).start()

    barrier = pltpu.get_barrier_semaphore()

    def greet(i, carry):
        pl.semaphore_signal(barrier, inc=1, **at(lax.rem(me + i, n)))
        return carry

    lax.fori_loop(1, n, greet, 0)

    zrow = jnp.zeros((PAD, nx), jnp.float32)
    for p in range(depth + 4):
        z[p, 0:PAD, :] = zrow
        z[p, ny + PAD : ny + 2 * PAD, :] = zrow
    for p in range(depth + 2):
        y[p, 0:PAD, :] = zrow
        y[p, ny + PAD : ny + 2 * PAD, :] = zrow
    for p in range(depth):
        v[p, ny : ny + PAD, :] = zrow
    acc[...] = jnp.zeros_like(acc)

    def zero_planes(ref, planes, offset):
        def body(i, carry):
            for p in planes:
                ref[p, pl.ds(pl.multiple_of(i * ROWS + offset, 8), ROWS), :] = jnp.zeros((ROWS, nx), jnp.float32)
            return carry
        lax.fori_loop(0, nb, body, 0)

    ob_in.wait()
    pl.semaphore_wait(barrier, n - 1)

    ob_down = pltpu.make_async_remote_copy(
        ob.at[pl.ds(2, 2)], ob.at[pl.ds(depth + 2, 2)], ob_send.at[0], ob_recv.at[0], **at(low))
    ob_up = pltpu.make_async_remote_copy(
        ob.at[pl.ds(depth, 2)], ob.at[pl.ds(0, 2)], ob_send.at[1], ob_recv.at[1], **at(high))

    @pl.when(has_low)
    def _():
        ob_down.start()

    @pl.when(has_high)
    def _():
        ob_up.start()

    @pl.when(jnp.logical_not(has_low))
    def _():
        ob[0:2] = jnp.zeros((2,) + ob.shape[1:], jnp.int32)
        zero_planes(z, (0, 1), PAD)

    @pl.when(jnp.logical_not(has_high))
    def _():
        ob[depth + 2 : depth + 4] = jnp.zeros((2,) + ob.shape[1:], jnp.int32)
        zero_planes(z, (depth + 2, depth + 3), PAD)
        zero_planes(lw_next, (0,), 0)

    mx[...] = jnp.zeros_like(mx)
    for k in range(3):
        ref = ins[k][1]
        for p in range(depth):
            load(k, p).wait()

            def body(i, m, ref=ref, p=p):
                a = jnp.abs(ref[p, pl.ds(pl.multiple_of(i * ROWS, 8), ROWS), :])
                return jnp.maximum(m, jnp.max(a.reshape(ROWS // 8, 8, nx), axis=0))

            m = lax.fori_loop(0, nb, body, jnp.zeros((8, nx), jnp.float32))
            m = jnp.max(m, axis=0, keepdims=True)
            for c in range(0, nx, 128):
                mx[...] = jnp.maximum(mx[...], jnp.broadcast_to(m[:, c : c + 128], mx.shape))

    def spread(src, dst, send, recv):
        def copy(i):
            return pltpu.make_async_remote_copy(
                src, dst.at[i], send.at[i], recv.at[i], **at(lax.rem(me + i, n)))

        def start(i, carry):
            copy(i).start()
            return carry

        def wait(i, carry):
            copy(i).wait_recv()
            copy(i).wait_send()
            return carry

        return (lambda: lax.fori_loop(1, n, start, 0)), (lambda: lax.fori_loop(1, n, wait, 0))

    mx_start, mx_wait = spread(mx, mx_all, mx_send, mx_recv)
    mx_start()

    @pl.when(has_low)
    def _():
        ob_down.wait_send()
        ob_up.wait_recv()

    @pl.when(has_high)
    def _():
        ob_up.wait_send()
        ob_down.wait_recv()

    row_id = lax.broadcasted_iota(jnp.int32, (nb, nx), 0)
    col_id = lax.broadcasted_iota(jnp.int32, (nb, nx), 1)
    srl = lax.shift_right_logical
    c1, c31 = jnp.int32(1), jnp.int32(31)
    full1, full31 = jnp.full((nb, nx), c1), jnp.full((nb, nx), c31)
    for p in range(depth + 2):
        mid = ob[p + 1]
        after = jnp.where(row_id == nb - 1, 0, pltpu.roll(mid, nb - 1, 0))
        before = jnp.where(row_id == 0, 0, pltpu.roll(mid, 1, 0))
        a = srl(mid, full1) | (after << full31)
        b = (mid << full1) | srl(before, full31)
        c = jnp.where(col_id == nx - 1, 0, pltpu.roll(mid, nx - 1, 1))
        d = jnp.where(col_id == 0, 0, pltpu.roll(mid, 1, 1))
        e, f = ob[p], ob[p + 2]
        s1, k1 = a ^ b ^ c, (a & b) | (c & (a | b))
        s2, k2 = d ^ e ^ f, (d & e) | (f & (d | e))
        k3 = s1 & s2
        cw[p, 0] = s1 ^ s2
        cw[p, 1] = k1 ^ k2 ^ k3
        cw[p, 2] = (k1 & k2) | (k3 & (k1 | k2))
        outside = None
        if p == 0:
            outside = jnp.logical_not(has_low)
        if p == depth + 1:
            outside = jnp.logical_not(has_high)
        cw[p, 3] = mid
        if outside is not None:
            @pl.when(outside)
            def _(p=p):
                cw[p, 3] = jnp.full((nb, nx), -1, jnp.int32)

    half = 16
    places = lax.broadcasted_iota(jnp.int32, (half, nx), 0)

    def code_rows(b, carry):
        for p in range(depth + 2):
            for k0 in range(0, ROWS, half):
                bits = [
                    srl(jnp.broadcast_to(cw[p, j, pl.ds(b, 1), :], (half, nx)), places + k0) & 1
                    for j in range(4)
                ]
                count = bits[0] + (bits[1] << 1) + (bits[2] << 2)
                code[p, pl.ds(pl.multiple_of(b * ROWS + k0, 8), half), :] = jnp.where(
                    bits[3] == 1, -1, 6 - count).astype(jnp.float32)
        return carry

    for p in range(depth):
        load(3, p).wait()
    mx_wait()
    mx_all[0] = mx[...]
    top = jnp.max(jnp.max(mx_all[...], axis=0), axis=1, keepdims=True)[0:1]
    top = jnp.broadcast_to(top, (1, nx))
    cf[0:1, :] = (CFL / (top + EPS)) * BUOYANCY

    lane = lax.broadcasted_iota(jnp.int32, (ROWS, nx), 1)

    def lifted(p, r):
        rows = pl.ds(r, ROWS)
        return w[p, rows, :] + cf[0:1, :] * s[p, rows, :]

    def chunked(prepare, compute, sends):
        def body(c, carry):
            @pl.when(c < chunks)
            def _():
                prepare(c)

                def inner(i, k):
                    compute(pl.multiple_of(c * crow + i * ROWS, 8))
                    return k
                lax.fori_loop(0, crow // ROWS, inner, 0)

            @pl.when(c > 0)
            def _():
                for cond, copy in sends:
                    @pl.when(cond)
                    def _(copy=copy):
                        copy(c - 1)
            return carry
        lax.fori_loop(0, chunks + 1, body, 0)

    def lw_copy(c):
        rows = pl.ds(pl.multiple_of(c * crow, 8), crow)
        return pltpu.make_async_remote_copy(
            lw.at[0, rows], lw_next.at[0, rows], lw_send.at[c], lw_recv.at[c], **at(low))

    def lw_rows(r):
        lw[0, pl.ds(r, ROWS), :] = lifted(0, r)

    chunked(lambda c: None, lw_rows, [(has_low, lambda c: lw_copy(c).start())])
    lax.fori_loop(0, nb, code_rows, 0)

    def z_copy(src, dst, send, recv, base, device):
        def copy(c):
            rows = pl.ds(pl.multiple_of(c * crow + PAD, 8), crow)
            return pltpu.make_async_remote_copy(
                z.at[src, rows], z.at[dst, rows], send.at[base + c], recv.at[base + c], **at(device))
        return copy

    down = [z_copy(2 + j, depth + 2 + j, dn_send, dn_recv, j * chunks, low) for j in range(2)]
    up = [z_copy(depth + j, j, up_send, up_recv, j * chunks, high) for j in range(2)]

    def z_rows(p, r):
        rows = pl.ds(r, ROWS)
        a = u[p, rows, :]
        flat = jnp.where(lane == nx - 1, 0.0, pltpu.roll(a, nx - 1, 1)) - a
        b = v[p, pl.ds(r, ROWS + PAD), :]
        flat = flat + (b[1 : ROWS + 1] - b[:ROWS])
        above = lifted(p + 1, r) if p + 1 < depth else lw_next[0, rows, :]
        own = lw[0, rows, :] if p == 0 else lifted(p, r)
        div = flat + (above - own)
        k = code[p + 1, rows, :]
        z[p + 2, pl.ds(pl.multiple_of(r + PAD, 8), ROWS), :] = (
            jnp.where(k >= 0.0, div, 0.0) / jnp.maximum(k, 1.0))

    def gated(before, copy):
        def start(c):
            before(c).wait_send()
            copy(c).start()
        return start

    top_plane = [] if depth > 2 else [(has_high, lambda c: up[0](c).start())]
    chunked(lambda c: None, functools.partial(z_rows, 0), top_plane)
    for p in range(1, depth - 1):
        sends = [(has_high, lambda c: up[0](c).start())] if p == depth - 2 else []
        chunked(lambda c: None, functools.partial(z_rows, p), sends)

    def above_wait(c):
        @pl.when(has_high)
        def _():
            lw_copy(c).wait_recv()

    chunked(above_wait, functools.partial(z_rows, depth - 1),
            [(has_high, gated(up[0], up[1])), (has_low, gated(lw_copy, down[0]))])

    def wait_all(cond, copy):
        def body(c, carry):
            @pl.when(cond)
            def _():
                copy(c).wait_recv()
            return carry
        lax.fori_loop(0, chunks, body, 0)

    def image(ref, slot, zm, zp, r, k):
        x = ref[slot, pl.ds(r, ROWS + 2 * PAD), :]
        mid = x[PAD : PAD + ROWS]
        beside = x[PAD + 1 : PAD + 1 + ROWS] + x[PAD - 1 : PAD - 1 + ROWS]
        beside = beside + jnp.where(lane == nx - 1, 0.0, pltpu.roll(mid, nx - 1, 1))
        beside = beside + jnp.where(lane == 0, 0.0, pltpu.roll(mid, 1, 1))
        beside = beside + zm + zp
        return mid, jnp.where(k >= 0.0, k * mid - beside, mid)

    def add(j, x):
        acc[j] += jnp.sum(x.reshape(ROWS // 8, 8, nx), axis=0)

    def y_rows(p, r):
        inner = pl.ds(pl.multiple_of(r + PAD, 8), ROWS)
        k = code[p + 1, pl.ds(r, ROWS), :]
        mid, q = image(z, p + 2, z[p + 1, inner, :], z[p + 3, inner, :], r, k)
        scaling = jnp.maximum(k, 1.0)
        out = q / scaling
        y[p + 1, inner, :] = out
        if 0 <= p < depth:
            d = scaling * mid
            add(0, d * mid)
            add(1, d * d)
            add(2, jnp.where(k >= 0.0, 1.0, 0.0))
            add(3, mid * q)
            add(4, q * out)

    def a_rows(p, r):
        inner = pl.ds(pl.multiple_of(r + PAD, 8), ROWS)
        k = code[p + 1, pl.ds(r, ROWS), :]
        mid, q = image(y, p + 1, y[p, inner, :], y[p + 2, inner, :], r, k)
        ay[p, pl.ds(r, ROWS), :] = q
        add(5, mid * q)

    def sweep(fn):
        def body(i, carry):
            fn(pl.multiple_of(i * ROWS, 8))
            return carry
        lax.fori_loop(0, nb, body, 0)

    for p in range(1, depth - 1):
        sweep(functools.partial(y_rows, p))
    wait_all(has_low, up[0])

    def push(c, carry):
        @pl.when(has_low)
        def _():
            gated(down[0], down[1])(c)
        return carry

    lax.fori_loop(0, chunks, push, 0)

    def middle(c, carry):
        def over(c, fn):
            def inner(i, k):
                fn(pl.multiple_of(c * crow + i * ROWS, 8))
                return k
            lax.fori_loop(0, crow // ROWS, inner, 0)

        def ahead(r):
            for p in sorted({0, depth - 1, depth}):
                y_rows(p, r)

        def behind(r):
            y_rows(-1, r)
            for p in range(depth):
                a_rows(p, r)

        @pl.when(c < chunks)
        def _():
            @pl.when(has_low)
            def _():
                up[1](c).wait_recv()

            @pl.when(has_high)
            def _():
                down[1](c).wait_recv()

                @pl.when(c == 0)
                def _():
                    down[0](0).wait_recv()

                @pl.when(c + 1 < chunks)
                def _():
                    down[0](c + 1).wait_recv()

            over(c, ahead)

        @pl.when(c > 0)
        def _():
            over(c - 1, behind)
        return carry

    lax.fori_loop(0, chunks + 1, middle, 0)

    for j in range(6):
        t = jnp.sum(acc[j], axis=0, keepdims=True)
        part = t[:, 0:128]
        for c in range(128, nx, 128):
            part = part + t[:, c : c + 128]
        st[j : j + 1, :] = part
    st[6:8, :] = jnp.zeros((2, 128), jnp.float32)
    st_start, st_wait = spread(st, st_all, st_send, st_recv)
    st_start()

    def drain(c, carry):
        @pl.when(has_low)
        def _():
            down[1](c).wait_send()

        @pl.when(has_high)
        def _():
            up[1](c).wait_send()
        return carry

    lax.fori_loop(0, chunks, drain, 0)
    st_wait()
    st_all[0] = st[...]
    total = jnp.sum(jnp.sum(st_all[...], axis=0), axis=1, keepdims=True)
    total = jnp.broadcast_to(total, (8, nx))
    gamma, squares, fluid = total[0:1], total[1:2], total[2:3]
    delta, eta, theta = total[3:4], total[4:5], total[5:6]
    alpha = gamma / delta
    gamma_next = gamma - 2.0 * alpha * delta + alpha * alpha * eta
    beta = gamma_next / gamma
    mixed = delta - alpha * eta
    curve = (delta - 2.0 * alpha * eta + alpha * alpha * theta) + 2.0 * beta * mixed + beta * beta * delta
    alpha_next = gamma_next / curve
    cf[1:2, :] = alpha + alpha_next * (1.0 + beta)
    cf[2:3, :] = alpha * alpha_next
    cf[3:4, :] = 1.0 / jnp.sqrt(squares / jnp.maximum(fluid, 1.0) + EPS)

    def out_copy(p, c, j):
        rows = pl.ds(pl.multiple_of(c * crow, 8), crow)
        src, dst = ((w, imp_hbm), (s, res_hbm))[j]
        return pltpu.make_async_copy(src.at[p, rows], dst.at[p, rows], out_sem.at[j * depth + p, c])

    for p in range(depth):
        def out_rows(r, p=p):
            inner = pl.ds(pl.multiple_of(r + PAD, 8), ROWS)
            rows = pl.ds(r, ROWS)
            zz, yy = z[p + 2, inner, :], y[p + 1, inner, :]
            scaling = jnp.maximum(code[p + 1, rows, :], 1.0)
            a, b = cf[1:2, :], cf[2:3, :]
            w[p, rows, :] = a * zz - b * yy
            s[p, rows, :] = (scaling * (zz - a * yy) + b * ay[p, rows, :]) * cf[3:4, :]

        chunked(lambda c: None, out_rows,
                [(True, lambda c, p=p: out_copy(p, c, 0).start()), (True, lambda c, p=p: out_copy(p, c, 1).start())])

    def finish(c, carry):
        for p in range(depth):
            for j in range(2):
                out_copy(p, c, j).wait()
        return carry

    lax.fori_loop(0, chunks, finish, 0)


def solution(mesh):
    n = mesh.shape["gz"]

    def local(u_face, v_face, w_face, smoke, obstacles):
        depth, ny, nx = u_face.shape
        nw = obstacles.shape[1]
        chunks = 8
        f32, i32 = jnp.float32, jnp.int32
        dma = pltpu.SemaphoreType.DMA
        any_spec = pl.BlockSpec(memory_space=pl.ANY)
        shape = jax.ShapeDtypeStruct((depth, ny, nx), f32)
        return pl.pallas_call(
            functools.partial(kernel, n, chunks),
            out_shape=(shape, shape),
            in_specs=[any_spec] * 5,
            out_specs=(any_spec, any_spec),
            scratch_shapes=[
                pltpu.VMEM((depth, ny, nx), f32),
                pltpu.VMEM((depth, ny + PAD, nx), f32),
                pltpu.VMEM((depth, ny, nx), f32),
                pltpu.VMEM((depth, ny, nx), f32),
                pltpu.VMEM((depth + 4, ny + 2 * PAD, nx), f32),
                pltpu.VMEM((depth + 2, ny + 2 * PAD, nx), f32),
                pltpu.VMEM((depth + 2, ny, nx), f32),
                pltpu.VMEM((depth, ny, nx), f32),
                pltpu.VMEM((1, ny, nx), f32),
                pltpu.VMEM((1, ny, nx), f32),
                pltpu.VMEM((depth + 4, nw, nx), i32),
                pltpu.VMEM((depth + 2, 4, nw, nx), i32),
                pltpu.VMEM((6, 8, nx), f32),
                pltpu.VMEM((8, nx), f32),
                pltpu.VMEM((8, 128), f32),
                pltpu.VMEM((n, 8, 128), f32),
                pltpu.VMEM((8, 128), f32),
                pltpu.VMEM((n, 8, 128), f32),
                dma((4 * depth + 1,)),
                dma((2,)), dma((2,)),
                dma((chunks,)), dma((chunks,)),
                dma((2 * chunks,)), dma((2 * chunks,)),
                dma((2 * chunks,)), dma((2 * chunks,)),
                dma((n,)), dma((n,)),
                dma((n,)), dma((n,)),
                dma((2 * depth, chunks)),
            ],
            compiler_params=pltpu.CompilerParams(
                collective_id=0, has_side_effects=True, vmem_limit_bytes=66_000_000),
            name="smoke_step",
        )(u_face, v_face, w_face, smoke, obstacles)

    placed = P("gz", None, None)
    return jax.shard_map(local, mesh=mesh, in_specs=(placed,) * 5, out_specs=(placed, placed), check_vma=False)
```

```python
import functools

import jax
import jax.numpy as jnp
from jax import lax
from jax.experimental import pallas as pl
from jax.experimental.pallas import tpu as pltpu
from jax.sharding import PartitionSpec as P

EPS = 1e-06
CFL = 0.5
BUOYANCY = 100.0

ROWS = 32
PAD = 8


def kernel(n, chunks, u_hbm, v_hbm, w_hbm, s_hbm, ob_hbm, z_out, y_out, code_out, ay_out, cf_out,
           u, v, w, s, z, y, code, ay, lw, lw_next, ob, cw, acc, cf, mx, mx_all, st, st_all,
           in_sem, ob_send, ob_recv, lw_send, lw_recv, dn_send, dn_recv, up_send, up_recv,
           mx_send, mx_recv, st_send, st_recv, out_sem):
    depth, ny, nx = w.shape
    nb = ny // ROWS
    crow = ny // chunks
    me = lax.axis_index("gz")
    has_low, has_high = me > 0, me < n - 1
    low, high = jnp.maximum(me - 1, 0), jnp.minimum(me + 1, n - 1)

    def at(device):
        return dict(device_id=(device,), device_id_type=pl.DeviceIdType.MESH)

    ins = [(u_hbm, u), (v_hbm, v), (w_hbm, w), (s_hbm, s)]

    def load(k, p):
        src, dst = ins[k]
        return pltpu.make_async_copy(src.at[p], dst.at[p, pl.ds(0, ny)], in_sem.at[k * depth + p])

    ob_in = pltpu.make_async_copy(ob_hbm, ob.at[pl.ds(2, depth)], in_sem.at[4 * depth])
    ob_in.start()
    for k in range(4):
        for p in range(depth):
            load(k, p).start()

    barrier = pltpu.get_barrier_semaphore()

    def greet(i, carry):
        pl.semaphore_signal(barrier, inc=1, **at(lax.rem(me + i, n)))
        return carry

    lax.fori_loop(1, n, greet, 0)

    zrow = jnp.zeros((PAD, nx), jnp.float32)
    for p in range(depth + 4):
        z[p, 0:PAD, :] = zrow
        z[p, ny + PAD : ny + 2 * PAD, :] = zrow
    for p in range(depth + 2):
        y[p, 0:PAD, :] = zrow
        y[p, ny + PAD : ny + 2 * PAD, :] = zrow
    for p in range(depth):
        v[p, ny : ny + PAD, :] = zrow
    acc[...] = jnp.zeros_like(acc)
    cf[...] = jnp.zeros_like(cf)

    def zero_planes(ref, planes, offset):
        def body(i, carry):
            for p in planes:
                ref[p, pl.ds(pl.multiple_of(i * ROWS + offset, 8), ROWS), :] = jnp.zeros((ROWS, nx), jnp.float32)
            return carry
        lax.fori_loop(0, nb, body, 0)

    ob_in.wait()
    pl.semaphore_wait(barrier, n - 1)

    ob_down = pltpu.make_async_remote_copy(
        ob.at[pl.ds(2, 2)], ob.at[pl.ds(depth + 2, 2)], ob_send.at[0], ob_recv.at[0], **at(low))
    ob_up = pltpu.make_async_remote_copy(
        ob.at[pl.ds(depth, 2)], ob.at[pl.ds(0, 2)], ob_send.at[1], ob_recv.at[1], **at(high))

    @pl.when(has_low)
    def _():
        ob_down.start()

    @pl.when(has_high)
    def _():
        ob_up.start()

    @pl.when(jnp.logical_not(has_low))
    def _():
        ob[0:2] = jnp.zeros((2,) + ob.shape[1:], jnp.int32)
        zero_planes(z, (0, 1), PAD)

    @pl.when(jnp.logical_not(has_high))
    def _():
        ob[depth + 2 : depth + 4] = jnp.zeros((2,) + ob.shape[1:], jnp.int32)
        zero_planes(z, (depth + 2, depth + 3), PAD)
        zero_planes(lw_next, (0,), 0)

    mx[...] = jnp.zeros_like(mx)
    for k in range(3):
        ref = ins[k][1]
        for p in range(depth):
            load(k, p).wait()

            def body(i, m, ref=ref, p=p):
                a = jnp.abs(ref[p, pl.ds(pl.multiple_of(i * ROWS, 8), ROWS), :])
                return jnp.maximum(m, jnp.max(a.reshape(ROWS // 8, 8, nx), axis=0))

            m = lax.fori_loop(0, nb, body, jnp.zeros((8, nx), jnp.float32))
            m = jnp.max(m, axis=0, keepdims=True)
            for c in range(0, nx, 128):
                mx[...] = jnp.maximum(mx[...], jnp.broadcast_to(m[:, c : c + 128], mx.shape))

    def spread(src, dst, send, recv):
        def copy(i):
            return pltpu.make_async_remote_copy(
                src, dst.at[i], send.at[i], recv.at[i], **at(lax.rem(me + i, n)))

        def start(i, carry):
            copy(i).start()
            return carry

        def wait(i, carry):
            copy(i).wait_recv()
            copy(i).wait_send()
            return carry

        return (lambda: lax.fori_loop(1, n, start, 0)), (lambda: lax.fori_loop(1, n, wait, 0))

    mx_start, mx_wait = spread(mx, mx_all, mx_send, mx_recv)
    mx_start()

    @pl.when(has_low)
    def _():
        ob_down.wait_send()
        ob_up.wait_recv()

    @pl.when(has_high)
    def _():
        ob_up.wait_send()
        ob_down.wait_recv()

    row_id = lax.broadcasted_iota(jnp.int32, (nb, nx), 0)
    col_id = lax.broadcasted_iota(jnp.int32, (nb, nx), 1)
    srl = lax.shift_right_logical
    c1, c31 = jnp.int32(1), jnp.int32(31)
    full1, full31 = jnp.full((nb, nx), c1), jnp.full((nb, nx), c31)
    for p in range(depth + 2):
        mid = ob[p + 1]
        after = jnp.where(row_id == nb - 1, 0, pltpu.roll(mid, nb - 1, 0))
        before = jnp.where(row_id == 0, 0, pltpu.roll(mid, 1, 0))
        a = srl(mid, full1) | (after << full31)
        b = (mid << full1) | srl(before, full31)
        c = jnp.where(col_id == nx - 1, 0, pltpu.roll(mid, nx - 1, 1))
        d = jnp.where(col_id == 0, 0, pltpu.roll(mid, 1, 1))
        e, f = ob[p], ob[p + 2]
        s1, k1 = a ^ b ^ c, (a & b) | (c & (a | b))
        s2, k2 = d ^ e ^ f, (d & e) | (f & (d | e))
        k3 = s1 & s2
        cw[p, 0] = s1 ^ s2
        cw[p, 1] = k1 ^ k2 ^ k3
        cw[p, 2] = (k1 & k2) | (k3 & (k1 | k2))
        outside = None
        if p == 0:
            outside = jnp.logical_not(has_low)
        if p == depth + 1:
            outside = jnp.logical_not(has_high)
        cw[p, 3] = mid
        if outside is not None:
            @pl.when(outside)
            def _(p=p):
                cw[p, 3] = jnp.full((nb, nx), -1, jnp.int32)

    half = 16
    places = lax.broadcasted_iota(jnp.int32, (half, nx), 0)

    def code_rows(b, carry):
        for p in range(depth + 2):
            for k0 in range(0, ROWS, half):
                bits = [
                    srl(jnp.broadcast_to(cw[p, j, pl.ds(b, 1), :], (half, nx)), places + k0) & 1
                    for j in range(4)
                ]
                count = bits[0] + (bits[1] << 1) + (bits[2] << 2)
                code[p, pl.ds(pl.multiple_of(b * ROWS + k0, 8), half), :] = jnp.where(
                    bits[3] == 1, -1, 6 - count).astype(jnp.float32)
        return carry

    for p in range(depth):
        load(3, p).wait()
    mx_wait()
    mx_all[0] = mx[...]
    top = jnp.max(jnp.max(mx_all[...], axis=0), axis=1, keepdims=True)[0:1]
    top = jnp.broadcast_to(top, (1, nx))
    cf[0:1, :] = (CFL / (top + EPS)) * BUOYANCY

    lane = lax.broadcasted_iota(jnp.int32, (ROWS, nx), 1)

    def lifted(p, r):
        rows = pl.ds(r, ROWS)
        return w[p, rows, :] + cf[0:1, :] * s[p, rows, :]

    def chunked(prepare, compute, sends):
        def body(c, carry):
            @pl.when(c < chunks)
            def _():
                prepare(c)

                def inner(i, k):
                    compute(pl.multiple_of(c * crow + i * ROWS, 8))
                    return k
                lax.fori_loop(0, crow // ROWS, inner, 0)

            @pl.when(c > 0)
            def _():
                for cond, copy in sends:
                    @pl.when(cond)
                    def _(copy=copy):
                        copy(c - 1)
            return carry
        lax.fori_loop(0, chunks + 1, body, 0)

    def lw_copy(c):
        rows = pl.ds(pl.multiple_of(c * crow, 8), crow)
        return pltpu.make_async_remote_copy(
            lw.at[0, rows], lw_next.at[0, rows], lw_send.at[c], lw_recv.at[c], **at(low))

    def lw_rows(r):
        lw[0, pl.ds(r, ROWS), :] = lifted(0, r)

    chunked(lambda c: None, lw_rows, [(has_low, lambda c: lw_copy(c).start())])
    lax.fori_loop(0, nb, code_rows, 0)

    def z_copy(src, dst, send, recv, base, device):
        def copy(c):
            rows = pl.ds(pl.multiple_of(c * crow + PAD, 8), crow)
            return pltpu.make_async_remote_copy(
                z.at[src, rows], z.at[dst, rows], send.at[base + c], recv.at[base + c], **at(device))
        return copy

    down = [z_copy(2 + j, depth + 2 + j, dn_send, dn_recv, j * chunks, low) for j in range(2)]
    up = [z_copy(depth + j, j, up_send, up_recv, j * chunks, high) for j in range(2)]

    def z_rows(p, r):
        rows = pl.ds(r, ROWS)
        a = u[p, rows, :]
        flat = jnp.where(lane == nx - 1, 0.0, pltpu.roll(a, nx - 1, 1)) - a
        b = v[p, pl.ds(r, ROWS + PAD), :]
        flat = flat + (b[1 : ROWS + 1] - b[:ROWS])
        above = lifted(p + 1, r) if p + 1 < depth else lw_next[0, rows, :]
        own = lw[0, rows, :] if p == 0 else lifted(p, r)
        div = flat + (above - own)
        k = code[p + 1, rows, :]
        z[p + 2, pl.ds(pl.multiple_of(r + PAD, 8), ROWS), :] = (
            jnp.where(k >= 0.0, div, 0.0) / jnp.maximum(k, 1.0))

    def gated(before, copy):
        def start(c):
            before(c).wait_send()
            copy(c).start()
        return start

    top_plane = [] if depth > 2 else [(has_high, lambda c: up[0](c).start())]
    chunked(lambda c: None, functools.partial(z_rows, 0), top_plane)
    for p in range(1, depth - 1):
        sends = [(has_high, lambda c: up[0](c).start())] if p == depth - 2 else []
        chunked(lambda c: None, functools.partial(z_rows, p), sends)

    def above_wait(c):
        @pl.when(has_high)
        def _():
            lw_copy(c).wait_recv()

    chunked(above_wait, functools.partial(z_rows, depth - 1),
            [(has_high, gated(up[0], up[1])), (has_low, gated(lw_copy, down[0]))])

    def wait_all(cond, copy):
        def body(c, carry):
            @pl.when(cond)
            def _():
                copy(c).wait_recv()
            return carry
        lax.fori_loop(0, chunks, body, 0)

    def image(ref, slot, zm, zp, r, k):
        x = ref[slot, pl.ds(r, ROWS + 2 * PAD), :]
        mid = x[PAD : PAD + ROWS]
        beside = x[PAD + 1 : PAD + 1 + ROWS] + x[PAD - 1 : PAD - 1 + ROWS]
        beside = beside + jnp.where(lane == nx - 1, 0.0, pltpu.roll(mid, nx - 1, 1))
        beside = beside + jnp.where(lane == 0, 0.0, pltpu.roll(mid, 1, 1))
        beside = beside + zm + zp
        return mid, jnp.where(k >= 0.0, k * mid - beside, mid)

    def add(j, x):
        acc[j] += jnp.sum(x.reshape(ROWS // 8, 8, nx), axis=0)

    def y_rows(p, r):
        inner = pl.ds(pl.multiple_of(r + PAD, 8), ROWS)
        k = code[p + 1, pl.ds(r, ROWS), :]
        mid, q = image(z, p + 2, z[p + 1, inner, :], z[p + 3, inner, :], r, k)
        scaling = jnp.maximum(k, 1.0)
        out = q / scaling
        y[p + 1, inner, :] = out
        if 0 <= p < depth:
            d = scaling * mid
            add(0, d * mid)
            add(1, d * d)
            add(2, jnp.where(k >= 0.0, 1.0, 0.0))
            add(3, mid * q)
            add(4, q * out)

    def a_rows(p, r):
        inner = pl.ds(pl.multiple_of(r + PAD, 8), ROWS)
        k = code[p + 1, pl.ds(r, ROWS), :]
        mid, q = image(y, p + 1, y[p, inner, :], y[p + 2, inner, :], r, k)
        ay[p, pl.ds(r, ROWS), :] = q
        add(5, mid * q)

    def sweep(fn):
        def body(i, carry):
            fn(pl.multiple_of(i * ROWS, 8))
            return carry
        lax.fori_loop(0, nb, body, 0)

    for p in range(1, depth - 1):
        sweep(functools.partial(y_rows, p))
    wait_all(has_low, up[0])

    def push(c, carry):
        @pl.when(has_low)
        def _():
            gated(down[0], down[1])(c)
        return carry

    lax.fori_loop(0, chunks, push, 0)

    def middle(c, carry):
        def over(c, fn):
            def inner(i, k):
                fn(pl.multiple_of(c * crow + i * ROWS, 8))
                return k
            lax.fori_loop(0, crow // ROWS, inner, 0)

        def ahead(r):
            for p in sorted({0, depth - 1, depth}):
                y_rows(p, r)

        def behind(r):
            y_rows(-1, r)
            for p in range(depth):
                a_rows(p, r)

        @pl.when(c < chunks)
        def _():
            @pl.when(has_low)
            def _():
                up[1](c).wait_recv()

            @pl.when(has_high)
            def _():
                down[1](c).wait_recv()

                @pl.when(c == 0)
                def _():
                    down[0](0).wait_recv()

                @pl.when(c + 1 < chunks)
                def _():
                    down[0](c + 1).wait_recv()

            over(c, ahead)

        @pl.when(c > 0)
        def _():
            over(c - 1, behind)
        return carry

    lax.fori_loop(0, chunks + 1, middle, 0)

    for j in range(6):
        t = jnp.sum(acc[j], axis=0, keepdims=True)
        part = t[:, 0:128]
        for c in range(128, nx, 128):
            part = part + t[:, c : c + 128]
        st[j : j + 1, :] = part
    st[6:8, :] = jnp.zeros((2, 128), jnp.float32)
    st_start, st_wait = spread(st, st_all, st_send, st_recv)
    st_start()

    inner = pl.ds(PAD, ny)
    outs = [
        pltpu.make_async_copy(z.at[pl.ds(2, depth), inner], z_out, out_sem.at[0]),
        pltpu.make_async_copy(y.at[pl.ds(1, depth), inner], y_out, out_sem.at[1]),
        pltpu.make_async_copy(code.at[pl.ds(1, depth)], code_out, out_sem.at[2]),
        pltpu.make_async_copy(ay, ay_out, out_sem.at[3]),
    ]
    for copy in outs:
        copy.start()

    def drain(c, carry):
        @pl.when(has_low)
        def _():
            down[1](c).wait_send()

        @pl.when(has_high)
        def _():
            up[1](c).wait_send()
        return carry

    lax.fori_loop(0, chunks, drain, 0)
    st_wait()
    st_all[0] = st[...]
    total = jnp.sum(jnp.sum(st_all[...], axis=0), axis=1, keepdims=True)
    total = jnp.broadcast_to(total, (8, nx))
    gamma, squares, fluid = total[0:1], total[1:2], total[2:3]
    delta, eta, theta = total[3:4], total[4:5], total[5:6]
    alpha = gamma / delta
    gamma_next = gamma - 2.0 * alpha * delta + alpha * alpha * eta
    beta = gamma_next / gamma
    mixed = delta - alpha * eta
    curve = (delta - 2.0 * alpha * eta + alpha * alpha * theta) + 2.0 * beta * mixed + beta * beta * delta
    alpha_next = gamma_next / curve
    cf[1:2, :] = alpha + alpha_next * (1.0 + beta)
    cf[2:3, :] = alpha * alpha_next
    cf[3:4, :] = 1.0 / jnp.sqrt(squares / jnp.maximum(fluid, 1.0) + EPS)

    cf_copy = pltpu.make_async_copy(cf, cf_out, out_sem.at[4])
    cf_copy.start()
    cf_copy.wait()
    for copy in outs:
        copy.wait()


def solution(mesh):
    n = mesh.shape["gz"]

    def local(u_face, v_face, w_face, smoke, obstacles):
        depth, ny, nx = u_face.shape
        nw = obstacles.shape[1]
        chunks = 8
        f32, i32 = jnp.float32, jnp.int32
        dma = pltpu.SemaphoreType.DMA
        any_spec = pl.BlockSpec(memory_space=pl.ANY)
        shape = jax.ShapeDtypeStruct((depth, ny, nx), f32)
        z, y, code, ay, cf = pl.pallas_call(
            functools.partial(kernel, n, chunks),
            out_shape=(shape,) * 4 + (jax.ShapeDtypeStruct((8, nx), f32),),
            in_specs=[any_spec] * 5,
            out_specs=(any_spec,) * 5,
            scratch_shapes=[
                pltpu.VMEM((depth, ny, nx), f32),
                pltpu.VMEM((depth, ny + PAD, nx), f32),
                pltpu.VMEM((depth, ny, nx), f32),
                pltpu.VMEM((depth, ny, nx), f32),
                pltpu.VMEM((depth + 4, ny + 2 * PAD, nx), f32),
                pltpu.VMEM((depth + 2, ny + 2 * PAD, nx), f32),
                pltpu.VMEM((depth + 2, ny, nx), f32),
                pltpu.VMEM((depth, ny, nx), f32),
                pltpu.VMEM((1, ny, nx), f32),
                pltpu.VMEM((1, ny, nx), f32),
                pltpu.VMEM((depth + 4, nw, nx), i32),
                pltpu.VMEM((depth + 2, 4, nw, nx), i32),
                pltpu.VMEM((6, 8, nx), f32),
                pltpu.VMEM((8, nx), f32),
                pltpu.VMEM((8, 128), f32),
                pltpu.VMEM((n, 8, 128), f32),
                pltpu.VMEM((8, 128), f32),
                pltpu.VMEM((n, 8, 128), f32),
                dma((4 * depth + 1,)),
                dma((2,)), dma((2,)),
                dma((chunks,)), dma((chunks,)),
                dma((2 * chunks,)), dma((2 * chunks,)),
                dma((2 * chunks,)), dma((2 * chunks,)),
                dma((n,)), dma((n,)),
                dma((n,)), dma((n,)),
                dma((5,)),
            ],
            compiler_params=pltpu.CompilerParams(
                collective_id=0, has_side_effects=True, vmem_limit_bytes=66_000_000),
            name="smoke_step",
        )(u_face, v_face, w_face, smoke, obstacles)
        a, b, norm = cf[1, 0], cf[2, 0], cf[3, 0]
        impulse = a * z - b * y
        residual = (jnp.maximum(code, 1.0) * (z - a * y) + b * ay) * norm
        return impulse, residual

    placed = P("gz", None, None)
    return jax.shard_map(local, mesh=mesh, in_specs=(placed,) * 5, out_specs=(placed, placed), check_vma=False)
```
